256 devices in a mesh: row: 4 (over x), col: 16 (over z, core), depth: 4 (over y).
Axes of the slice: x: 4, y: 4, z: 8, core: 2. Of those that a mesh axis runs over, the one named last changes fastest.
Arguments:
- a_cols: float32 [32768, 1024], P(('row', 'col')), may hold values from -16 to 24, as said below
- past_panels: float32 [32768, 2048], P(('row', 'col'), 'depth'), may hold values from -1 to 1
Outputs:
- factor: float32 [32768, 1024], P(('row', 'col'))
The draws below stay inside these ranges and needn't reach their ends.
Inputs may be any that keep to these rules, and one draw needn't show every extreme that they name: a_cols minus past_panels times the transpose of the top 1024 rows of past_panels is the first 1024 columns of a symmetric positive definite matrix whose top block has eigenvalues between 2 and 12.
All inputs are finite; a program needn't handle non-finite values.
Results may differ from the reference program's by a relative error of at most 0.0001.
Values sent between devices are 32-bit elements.
No kernel may reach another device: no remote copies, remote signals or barrier semaphores. Data moves between devices by JAX's collectives and lax.ppermute only.
A program may use at most 64 MiB of HBM per device.

```python
import math
import jax
import jax.numpy as jnp
from jax import lax

NB = 512
STEPS = 2
ROWS = 32768
W = 1024
PAST = 2048


def shared_draw(key):
    spread = jnp.sqrt(jnp.float32(0.4) / PAST)
    past = jnp.clip(jax.random.normal(jax.random.fold_in(key, 11), (ROWS, PAST), jnp.float32), -5.0, 5.0) * spread
    basis = jnp.clip(jax.random.normal(jax.random.fold_in(key, 12), (ROWS, W), jnp.float32), -5.0, 5.0)
    extra = jnp.exp(jax.random.uniform(jax.random.fold_in(key, 13), (W,), jnp.float32, math.log(2.0), math.log(4.0)))
    dims = (((1,), (1,)), ((), ()))
    schur = lax.dot_general(basis, basis[:W], dims, precision=lax.Precision.HIGHEST, preferred_element_type=jnp.float32) / W
    schur = schur.at[:W].add(jnp.diag(extra))
    whole = lax.dot_general(past, past[:W], dims, precision=lax.Precision.HIGHEST, preferred_element_type=jnp.float32) + schur
    return (whole, past)


def draw_a_cols(key, part):
    return shared_draw(key)[0]


def draw_past_panels(key, part):
    return shared_draw(key)[1]


def setup_inputs(seed: int = 0) -> dict:
    key_of = jax.random.split(jax.random.key(seed), 3)
    a_cols = draw_a_cols(jax.random.fold_in(key_of[2], 71), 0)
    past_panels = draw_past_panels(jax.random.fold_in(key_of[2], 71), 0)
    return {"a_cols": a_cols, "past_panels": past_panels}


def outer_rows(left, right):
    return lax.dot_general(left.astype(jnp.float32), right.astype(jnp.float32), (((1,), (1,)), ((), ())), precision=lax.Precision.HIGHEST, preferred_element_type=jnp.float32)

def reference(a_cols, past_panels):
    result = jnp.zeros((ROWS, W), jnp.float32)
    row_ids = jnp.arange(ROWS, dtype=jnp.int32)[:, None]
    col_ids = jnp.arange(NB, dtype=jnp.int32)[None, :]
    for section in range(STEPS):
        start = section * NB
        summed = outer_rows(past_panels, past_panels[start:start + NB])
        if section > 0:
            summed = summed + outer_rows(result[:, :start], result[start:start + NB, :start])
        update = a_cols[:, start:start + NB] - summed
        diag_factor = jnp.linalg.cholesky(update[start:start + NB])
        solved = jax.scipy.linalg.solve_triangular(diag_factor, update.T, lower=True).T
        new_panel = jnp.where(row_ids >= start + col_ids, solved, jnp.float32(0.0))
        result = result.at[:, start:start + NB].set(new_panel)
    return result
```

```python
import jax, jax.numpy as jnp
from jax import lax
from jax.experimental import pallas as pl
from jax.experimental.pallas import tpu as pltpu
NB=512
H=256
CENTRE, RADIUS = 7.0, 5.0
CHEB = 6
NEWTON = 2

def dims(ta, tb):
    return (((0 if ta else 1,), (1 if tb else 0,)), ((), ()))

def dot1(a, b, ta=False, tb=False):
    return lax.dot_general(a, b, dims(ta, tb), preferred_element_type=jnp.float32)

def split(a):
    hi = a.astype(jnp.bfloat16)
    return hi, (a - hi.astype(jnp.float32)).astype(jnp.bfloat16)

def dot3(a, b, ta=False, tb=False):
    (ah, al), (bh, bl) = a, b
    return dot1(ah, bh, ta, tb) + (dot1(ah, bl, ta, tb) + dot1(al, bh, ta, tb))

def tri(n, strict=False):
    r = lax.broadcasted_iota(jnp.int32, (n, n), 0)
    c = lax.broadcasted_iota(jnp.int32, (n, n), 1)
    return (r > c) if strict else (r >= c)

def eye(n):
    r = lax.broadcasted_iota(jnp.int32, (n, n), 0)
    c = lax.broadcasted_iota(jnp.int32, (n, n), 1)
    return (r == c)

def inverse_factor(a00, a10, a11):
    b = jnp.bfloat16
    low, ident = tri(H), eye(H).astype(jnp.float32)
    h00, h10, h11 = split(a00), split(a10), split(a11)
    b00, b10, b11 = h00[0], h10[0], h11[0]
    sigma = CENTRE / RADIUS
    rho = 1.0 / sigma
    d00 = ident * (1.0 / CENTRE); d11 = d00; d10 = jnp.zeros((H, H), jnp.float32)
    y00, y10, y11 = d00, d10, d11
    zero = jnp.zeros((H, H), jnp.float32)
    r00 = ident - jnp.where(low, a00, 0.0) * (1.0 / CENTRE)
    r10 = -a10 * (1.0 / CENTRE)
    r11 = ident - jnp.where(low, a11, 0.0) * (1.0 / CENTRE)
    for k in range(CHEB):
        nxt = 1.0 / (2.0 * sigma - rho)
        p, q = nxt * rho, 2.0 * nxt / RADIUS
        rho = nxt
        d00, d10, d11 = p * d00 + q * r00, p * d10 + q * r10, p * d11 + q * r11
        y00, y10, y11 = y00 + d00, y10 + d10, y11 + d11
        if k < CHEB - 1:
            v00, v10, v11 = y00.astype(b), y10.astype(b), y11.astype(b)
            r00 = ident - jnp.where(low, dot1(v00, b00), 0.0)
            r10 = -(dot1(v10, b00) + dot1(v11, b10))
            r11 = ident - jnp.where(low, dot1(v10, b10, False, True) + dot1(v11, b11), 0.0)
    s0 = lax.rsqrt(jnp.sum(y00 * ident, axis=1, keepdims=True))
    s1 = lax.rsqrt(jnp.sum(y11 * ident, axis=1, keepdims=True))
    x00, x10, x11 = y00 * s0, y10 * s1, y11 * s1
    half = jnp.where(tri(H, True), 1.0, 0.5 * ident)
    for k in range(NEWTON):
        t00, t10, t11 = split(x00), split(x10), split(x11)
        w00 = split(dot3(t00, h00))
        w10 = split(dot3(t10, h00) + dot3(t11, h10))
        w11 = split(dot3(t10, h10, False, True) + dot3(t11, h11))
        e00 = ((dot3(w00, t00, False, True) - ident) * half).astype(b)
        e10 = dot3(w10, t00, False, True).astype(b)
        e11 = ((dot3(w10, t10, False, True) + dot3(w11, t11, False, True) - ident) * half).astype(b)
        x10 = x10 - (dot1(e10, t00[0]) + dot1(e11, t10[0]))
        x00 = x00 - dot1(e00, t00[0])
        x11 = x11 - dot1(e11, t11[0])
    return x00, x10, x11

def factor_kernel(m0, m1, x_ref, l_ref):
    def put(i, x00, x10, x11):
        x_ref[i, :H, :H] = x00
        x_ref[i, :H, H:] = jnp.zeros((H, H), jnp.float32)
        x_ref[i, H:, :H] = x10
        x_ref[i, H:, H:] = x11
    x00, x10, x11 = inverse_factor(m0[:H, :H], m0[H:, :H], m0[H:, H:NB])
    put(0, x00, x10, x11)
    t00, t10, t11 = split(x00), split(x10), split(x11)
    for j, m in enumerate((m0, m1)):
        top, bot = split(m[:H, NB:]), split(m[H:, NB:])
        l_ref[:H, j * H:(j + 1) * H] = dot3(t00, top)
        l_ref[H:, j * H:(j + 1) * H] = dot3(t10, top) + dot3(t11, bot)
    p0, p1 = split(l_ref[:, :H]), split(l_ref[:, H:])
    c00 = m1[:H, :H] - dot3(p0, p0, True, False)
    c10 = m1[H:, :H] - dot3(p1, p0, True, False)
    c11 = m1[H:, H:NB] - dot3(p1, p1, True, False)
    put(1, *inverse_factor(c00, c10, c11))

def factor(m0, m1):
    return pl.pallas_call(
        factor_kernel,
        out_shape=(jax.ShapeDtypeStruct((2, NB, NB), jnp.float32), jax.ShapeDtypeStruct((NB, NB), jnp.float32)),
        in_specs=[pl.BlockSpec(memory_space=pltpu.VMEM)] * 2,
        out_specs=(pl.BlockSpec(memory_space=pltpu.VMEM),) * 2,
        cost_estimate=pl.CostEstimate(flops=2 * 10**10, bytes_accessed=2**23, transcendentals=0),
        name="factor",
    )(m0, m1)


from jax.sharding import Mesh
from jax.sharding import PartitionSpec as P

ROW_COL = ("row", "col_0", "col_1")
PLANE = ("row", "col_0")


def outer_rows(left, right):
    return lax.dot_general(
        left, right, (((1,), (1,)), ((), ())), precision=lax.Precision.HIGH, preferred_element_type=jnp.float32
    )


def swap_core(v):
    return lax.ppermute(v, "col_1", [(0, 1), (1, 0)])


def exchange(v, axis, size, bits):
    return lax.ppermute(v, axis, [(i, i ^ bits) for i in range(size)])


def in_order(pieces, me):
    low, high = (me & 1) == 1, (me >> 1) == 1
    p0, p1, p2, p3 = pieces
    p0, p1 = jnp.where(low, p1, p0), jnp.where(low, p0, p1)
    p2, p3 = jnp.where(low, p3, p2), jnp.where(low, p2, p3)
    p0, p2 = jnp.where(high, p2, p0), jnp.where(high, p0, p2)
    p1, p3 = jnp.where(high, p3, p1), jnp.where(high, p1, p3)
    return jnp.concatenate([p0, p1, p2, p3])


def gather_four(v, axis):
    return in_order([v] + [exchange(v, axis, 4, s) for s in (1, 2, 3)], lax.axis_index(axis))


def chunk_of(v, j):
    n = v.shape[0] // 4
    return lax.dynamic_slice_in_dim(v, j * n, n)


def scatter_sum(v, axis):
    me = lax.axis_index(axis)
    total = chunk_of(v, me)
    for s in (1, 2, 3):
        total = total + exchange(chunk_of(v, me ^ s), axis, 4, s)
    return total


def broadcast_plane(v):
    x, z = lax.axis_index("row"), lax.axis_index("col_0")
    n = v.shape[0] // 4
    mine = jnp.where((x == 0) & (z == 0), v[:n], 0.0)
    for p in (1, 2, 3):
        mine = mine + lax.ppermute(v[p * n : (p + 1) * n], PLANE, [(0, 8 * p)])
    got = jnp.where(z == 0, mine, 0.0)
    for p in (4, 2, 6):
        got = got + lax.ppermute(mine, "col_0", [(0, p)])
    odd = lax.ppermute(got, "col_0", [(0, 1), (2, 3), (4, 5), (6, 7)])
    got = jnp.where(z % 2 == 0, got, odd)
    return gather_four(got, "row")


def body(a_cols, past):
    core, y = lax.axis_index("col_1"), lax.axis_index("depth")
    first = core == 0

    other = swap_core(past)
    diag = outer_rows(past, past)
    side = outer_rows(jnp.where(first, past, other), jnp.where(first, other[:H], past[H:]))
    a_diag = jnp.where(first, a_cols[:, :NB], a_cols[:, NB:])
    a_side = jnp.where(first, a_cols[:, NB : NB + H], a_cols[H:, :NB].T)
    block = chunk_of(jnp.concatenate([a_diag, a_side], 1), y) - scatter_sum(
        jnp.concatenate([diag, side], 1), "depth"
    )

    top = broadcast_plane(past)
    top_other = swap_core(top)

    block = gather_four(broadcast_plane(block), "depth")
    block_other = swap_core(block)
    inverse, below = factor(
        jnp.where(first, block, block_other), jnp.where(first, block_other, block)
    )

    partial_value = jnp.concatenate([outer_rows(past, top), outer_rows(past, top_other)], 1)
    a_turned = jnp.concatenate([a_diag, jnp.where(first, a_cols[:, NB:], a_cols[:, :NB])], 1)
    update = gather_four(chunk_of(a_turned, y) - scatter_sum(partial_value, "depth"), "depth")
    update_1 = jnp.where(first, update[:, :NB], update[:, NB:])
    update_2 = jnp.where(first, update[:, NB:], update[:, :NB])
    out_1 = outer_rows(update_1, inverse[0])
    rest = update_2 - lax.dot_general(
        out_1, below, (((1,), (0,)), ((), ())), precision=lax.Precision.HIGH, preferred_element_type=jnp.float32
    )
    out_2 = outer_rows(rest, inverse[1])
    out = jnp.concatenate([out_1, out_2], 1)
    rows = lax.axis_index(ROW_COL) * out.shape[0] + lax.broadcasted_iota(jnp.int32, out.shape, 0)
    return jnp.where(rows >= lax.broadcasted_iota(jnp.int32, out.shape, 1), out, 0.0)


def solution(mesh):
    split_mesh = Mesh(
        mesh.devices.reshape(mesh.shape["row"], 8, 2, mesh.shape["depth"]),
        ("row", "col_0", "col_1", "depth"),
    )
    placed = (P(ROW_COL, None), P(ROW_COL, "depth"))
    return jax.shard_map(
        body, mesh=split_mesh, in_specs=placed, out_specs=P(ROW_COL, None), check_vma=False
    )
```

```python
import jax, jax.numpy as jnp
from jax import lax
from jax.experimental import pallas as pl
from jax.experimental.pallas import tpu as pltpu
NB=512
H=256
CENTRE, RADIUS = 7.0, 5.0
CHEB = 6
NEWTON = 2


def dims(ta, tb):
    return (((0 if ta else 1,), (1 if tb else 0,)), ((), ()))


def dot1(a, b, ta=False, tb=False):
    return lax.dot_general(a, b, dims(ta, tb), preferred_element_type=jnp.float32)


def split(a):
    hi = a.astype(jnp.bfloat16)
    return hi, (a - hi.astype(jnp.float32)).astype(jnp.bfloat16)


def dot3(a, b, ta=False, tb=False):
    (ah, al), (bh, bl) = a, b
    return dot1(ah, bh, ta, tb) + (dot1(ah, bl, ta, tb) + dot1(al, bh, ta, tb))


def tri(n, strict=False):
    r = lax.broadcasted_iota(jnp.int32, (n, n), 0)
    c = lax.broadcasted_iota(jnp.int32, (n, n), 1)
    return (r > c) if strict else (r >= c)


def eye(n):
    r = lax.broadcasted_iota(jnp.int32, (n, n), 0)
    c = lax.broadcasted_iota(jnp.int32, (n, n), 1)
    return (r == c)


def inverse_factor(a00, a10, a11):
    b = jnp.bfloat16
    low, ident = tri(H), eye(H).astype(jnp.float32)
    h00, h10, h11 = split(a00), split(a10), split(a11)
    b00, b10, b11 = h00[0], h10[0], h11[0]
    sigma = CENTRE / RADIUS
    rho = 1.0 / sigma
    d00 = ident * (1.0 / CENTRE); d11 = d00; d10 = jnp.zeros((H, H), jnp.float32)
    y00, y10, y11 = d00, d10, d11
    zero = jnp.zeros((H, H), jnp.float32)
    r00 = ident - jnp.where(low, a00, 0.0) * (1.0 / CENTRE)
    r10 = -a10 * (1.0 / CENTRE)
    r11 = ident - jnp.where(low, a11, 0.0) * (1.0 / CENTRE)
    for k in range(CHEB):
        nxt = 1.0 / (2.0 * sigma - rho)
        p, q = nxt * rho, 2.0 * nxt / RADIUS
        rho = nxt
        d00, d10, d11 = p * d00 + q * r00, p * d10 + q * r10, p * d11 + q * r11
        y00, y10, y11 = y00 + d00, y10 + d10, y11 + d11
        if k < CHEB - 1:
            v00, v10, v11 = y00.astype(b), y10.astype(b), y11.astype(b)
            r00 = ident - jnp.where(low, dot1(v00, b00), 0.0)
            r10 = -(dot1(v10, b00) + dot1(v11, b10))
            r11 = ident - jnp.where(low, dot1(v10, b10, False, True) + dot1(v11, b11), 0.0)
    s0 = lax.rsqrt(jnp.sum(y00 * ident, axis=1, keepdims=True))
    s1 = lax.rsqrt(jnp.sum(y11 * ident, axis=1, keepdims=True))
    x00, x10, x11 = y00 * s0, y10 * s1, y11 * s1
    half = jnp.where(tri(H, True), 1.0, 0.5 * ident)
    for _ in range(NEWTON):
        t00, t10, t11 = split(x00), split(x10), split(x11)
        w00 = split(dot3(t00, h00))
        w10 = split(dot3(t10, h00) + dot3(t11, h10))
        w11 = split(dot3(t10, h10, False, True) + dot3(t11, h11))
        e00 = ((dot3(w00, t00, False, True) - ident) * half).astype(b)
        e10 = dot3(w10, t00, False, True).astype(b)
        e11 = ((dot3(w10, t10, False, True) + dot3(w11, t11, False, True) - ident) * half).astype(b)
        x10 = x10 - (dot1(e10, t00[0]) + dot1(e11, t10[0]))
        x00 = x00 - dot1(e00, t00[0])
        x11 = x11 - dot1(e11, t11[0])
    return x00, x10, x11


VMEM = pl.BlockSpec(memory_space=pltpu.VMEM)
SMEM = pl.BlockSpec(memory_space=pltpu.SMEM)
F32 = jnp.float32


def block_kernel(where_ref, own, other, a_ref, *refs):
    outs, part, a_part = refs[:4], refs[4], refs[5]
    first, y = where_ref[0] == 0, where_ref[1]
    t0, t1 = split(own[:H, :]), split(own[H:, :])
    part[:, :H] = -dot3(t0, t0, False, True)
    part[:, H : 2 * H] = -dot3(t1, t0, False, True)
    part[:, 2 * H : 3 * H] = -dot3(t1, t1, False, True)

    @pl.when(first)
    def _():
        q = split(other[:H, :])
        part[:, 3 * H : 4 * H] = -dot3(t0, q, False, True)
        part[:, 4 * H :] = -dot3(t1, q, False, True)
        a_part[:, :H] = a_ref[:H, :H]
        a_part[:, H : 2 * H] = a_ref[H:, :H]
        a_part[:, 2 * H : 3 * H] = a_ref[H:, H:NB]
        a_part[:, 3 * H : 4 * H] = a_ref[:H, NB : NB + H]
        a_part[:, 4 * H :] = a_ref[H:, NB : NB + H]

    @pl.when(jnp.logical_not(first))
    def _():
        part[:, 3 * H : 4 * H] = -dot3(split(other[:H, :]), t1, False, True)
        part[:, 4 * H :] = -dot3(split(other[H:, :]), t1, False, True)
        a_part[:, :H] = a_ref[:H, NB : NB + H]
        a_part[:, H : 2 * H] = a_ref[H:, NB : NB + H]
        a_part[:, 2 * H : 3 * H] = a_ref[H:, NB + H :]
        a_part[:, 3 * H : 4 * H] = a_ref[H:, :H].T
        a_part[:, 4 * H :] = a_ref[H:, H:NB].T

    n = H // 4
    outs[0][...] = part[pl.ds(y * n, n), :] + a_part[pl.ds(y * n, n), :]
    for s in (1, 2, 3):
        outs[s][...] = part[pl.ds((y ^ s) * n, n), :]


def block_parts(where, own, other, a_cols):
    return pl.pallas_call(
        block_kernel,
        out_shape=(jax.ShapeDtypeStruct((H // 4, 5 * H), F32),) * 4,
        in_specs=[SMEM, VMEM, VMEM, VMEM],
        out_specs=(VMEM,) * 4,
        scratch_shapes=[pltpu.VMEM((H, 5 * H), F32)] * 2,
        cost_estimate=pl.CostEstimate(flops=10**9, bytes_accessed=2**22, transcendentals=0),
        name="block_parts",
    )(where, own, other, a_cols)


def factor_kernel(where_ref, own, other, x_ref, l_ref, m0, m1):
    @pl.when(where_ref[0] == 0)
    def _():
        m0[...] = own[...]
        m1[...] = other[...]

    @pl.when(where_ref[0] != 0)
    def _():
        m0[...] = other[...]
        m1[...] = own[...]

    def tile(m, i):
        return m[:, i * H : (i + 1) * H]

    def put(i, x00, x10, x11):
        x_ref[i, :H, :H] = x00
        x_ref[i, :H, H:] = jnp.zeros((H, H), F32)
        x_ref[i, H:, :H] = x10
        x_ref[i, H:, H:] = x11

    x00, x10, x11 = inverse_factor(tile(m0, 0), tile(m0, 1), tile(m0, 2))
    put(0, x00, x10, x11)
    t00, t10, t11 = split(x00), split(x10), split(x11)
    for j, m in enumerate((m0, m1)):
        top, bot = split(tile(m, 3)), split(tile(m, 4))
        l_ref[:H, j * H : (j + 1) * H] = dot3(t00, top)
        l_ref[H:, j * H : (j + 1) * H] = dot3(t10, top) + dot3(t11, bot)
    p0, p1 = split(l_ref[:, :H]), split(l_ref[:, H:])
    c00 = tile(m1, 0) - dot3(p0, p0, True, False)
    c10 = tile(m1, 1) - dot3(p1, p0, True, False)
    c11 = tile(m1, 2) - dot3(p1, p1, True, False)
    put(1, *inverse_factor(c00, c10, c11))


def factor(where, own, other):
    return pl.pallas_call(
        factor_kernel,
        out_shape=(jax.ShapeDtypeStruct((2, NB, NB), F32), jax.ShapeDtypeStruct((NB, NB), F32)),
        in_specs=[SMEM] + [VMEM] * 2,
        out_specs=(VMEM,) * 2,
        scratch_shapes=[pltpu.VMEM((H, 5 * H), F32)] * 2,
        cost_estimate=pl.CostEstimate(flops=5 * 10**9, bytes_accessed=2**23, transcendentals=0),
        name="factor",
    )(where, own, other)


def update_kernel(where_ref, p0, p1, p2a, p2b, p3, own, other, a_ref, out, ph, pl_, th, tl):
    core, y = where_ref[0], where_ref[1]
    n = 128

    def put(hi, lo, rows, t, v):
        columns = slice(t * NB, (t + 1) * NB)
        hi[rows, columns], lo[rows, columns] = split(v)

    every = slice(0, NB)
    put(ph, pl_, every, 0, p0[...])
    put(ph, pl_, every, 1, p1[...])
    put(ph, pl_, slice(0, H), 2, p2a[...])
    put(ph, pl_, slice(H, NB), 2, p2b[...])
    put(ph, pl_, every, 3, p3[...])
    for t in range(4):
        put(th, tl, slice(0, n), t, own[t * n : (t + 1) * n, :])
        put(th, tl, slice(n, 2 * n), t, other[t * n : (t + 1) * n, :])
    total = dot3((ph[...], pl_[...]), (th[...], tl[...]), False, True)
    for i, half in enumerate((core, 1 - core)):
        columns = pl.ds(pl.multiple_of(half * NB + y * n, n), n)
        out[:, pl.ds(pl.multiple_of(half * n, n), n)] = a_ref[:, columns] - total[:, i * n : (i + 1) * n]


def update_part(where, past, own, other, a_cols):
    return pl.pallas_call(
        update_kernel,
        out_shape=jax.ShapeDtypeStruct((NB, 256), F32),
        in_specs=[SMEM] + [VMEM] * 8,
        out_specs=VMEM,
        scratch_shapes=[pltpu.VMEM((r, 4 * NB), jnp.bfloat16) for r in (NB, NB, H, H)],
        cost_estimate=pl.CostEstimate(flops=10**9, bytes_accessed=2**22, transcendentals=0),
        name="update_part",
    )(where, *past, own, other, a_cols)


def solve_kernel(where_ref, u0, u1, u2, u3, x_ref, l_ref, out, s1, s2):
    y, position = where_ref[1], where_ref[2]
    n = 128
    for u, piece in enumerate((u0, u1, u2, u3)):
        columns = pl.ds(pl.multiple_of((y ^ u) * n, n), n)
        s1[:, columns] = piece[:, :n]
        s2[:, columns] = piece[:, n:]

    def keep(v, start):
        rows = position * NB + lax.broadcasted_iota(jnp.int32, v.shape, 0)
        return jnp.where(rows >= start + lax.broadcasted_iota(jnp.int32, v.shape, 1), v, 0.0)

    def times_inverse(i, s, start):
        left, right = split(s[:, :H]), split(s[:, H:])
        a = dot3(left, split(x_ref[i, :H, :H]), False, True)
        b = dot3(left, split(x_ref[i, H:, :H]), False, True) + dot3(right, split(x_ref[i, H:, H:]), False, True)
        out[:, start : start + H] = keep(a, start)
        out[:, start + H : start + NB] = keep(b, start + H)
        return a, b

    a, b = times_inverse(0, s1, 0)
    a, b = split(a), split(b)
    s2[...] = s2[...] - (dot3(a, split(l_ref[:H, :])) + dot3(b, split(l_ref[H:, :])))
    times_inverse(1, s2, NB)


def solve(where, pieces, inverse, below):
    return pl.pallas_call(
        solve_kernel,
        out_shape=jax.ShapeDtypeStruct((NB, 2 * NB), F32),
        in_specs=[SMEM] + [VMEM] * 6,
        out_specs=VMEM,
        scratch_shapes=[pltpu.VMEM((NB, NB), F32)] * 2,
        cost_estimate=pl.CostEstimate(flops=10**9, bytes_accessed=2**22, transcendentals=0),
        name="solve",
    )(where, *pieces, inverse, below)


from jax.sharding import Mesh
from jax.sharding import PartitionSpec as P

ROW_COL = ("row", "col_0", "col_1")
PLANE = ("row", "col_0")
BOX = ("row", "col_0", "depth")
TRADE = False


def send(v, axis, pairs, one_way=False):
    if one_way and TRADE:
        pairs = pairs + [(b, a) for a, b in pairs]
    return lax.ppermute(v, axis, pairs)


def swap_core(v):
    return send(v, "col_1", [(0, 1), (1, 0)])


def exchange(v, axis, bits):
    return send(v, axis, [(i, i ^ bits) for i in range(4)])


def in_order(pieces, me):
    low, high = (me & 1) == 1, (me >> 1) == 1
    p0, p1, p2, p3 = pieces
    p0, p1 = jnp.where(low, p1, p0), jnp.where(low, p0, p1)
    p2, p3 = jnp.where(low, p3, p2), jnp.where(low, p2, p3)
    p0, p2 = jnp.where(high, p2, p0), jnp.where(high, p0, p2)
    p1, p3 = jnp.where(high, p3, p1), jnp.where(high, p1, p3)
    return jnp.concatenate([p0, p1, p2, p3])


def pieces_along(v, axis):
    return [v] + [exchange(v, axis, s) for s in (1, 2, 3)]


def chunk_of(v, j):
    n = v.shape[0] // 4
    return lax.dynamic_slice_in_dim(v, j * n, n)


def spread_z(v, z):
    a = send(v, "col_0", [(0, 3)], True) + send(v, "col_0", [(0, 5)], True)
    v = jnp.where(z == 0, v, a)
    b = send(v, "col_0", [(0, 1), (3, 4), (5, 6)], True) + send(v, "col_0", [(0, 7), (3, 2)], True)
    return jnp.where((z == 0) | (z == 3) | (z == 5), v, b)


def body(a_cols, past):
    x, z = lax.axis_index("row"), lax.axis_index("col_0")
    core, y = lax.axis_index("col_1"), lax.axis_index("depth")
    root = (x == 0) & (z == 0)
    where = jnp.stack([core, y, lax.axis_index(ROW_COL)]).astype(jnp.int32)

    other = swap_core(past)
    got = 0.0
    for s in (1, 2, 3):
        pairs = [(d, 32 * s + (d ^ s)) for d in range(4)]
        got = got + send(chunk_of(past, y ^ s), BOX, pairs, True)
    top = jnp.where(root, chunk_of(past, y), got)

    parts = block_parts(where, past, other, a_cols)
    block = parts[0]
    for s in (1, 2, 3):
        block = block + exchange(parts[s], "depth", s)

    near1, near3 = exchange(past, "depth", 1), exchange(past, "depth", 3)
    far = exchange(near3[:H], "depth", 1), exchange(near1[H:], "depth", 3)
    rows = past, near1, *far, near3

    top = in_order(pieces_along(spread_z(top, z), "row"), x)
    top_other = swap_core(top)

    n = block.shape[0] // 4
    got = 0.0
    for p in (1, 2, 3):
        got = got + send(block[p * n : (p + 1) * n], PLANE, [(0, 8 * p)], True)
    spread = spread_z(jnp.where(root, block[:n], got), z)
    spread = in_order(pieces_along(spread, "depth"), y).reshape(4, n, -1)
    spread = in_order(pieces_along(spread[None], "row"), x)
    block = spread.transpose(1, 0, 2, 3).reshape(H, -1)
    block_other = swap_core(block)

    update = update_part(where, rows, top, top_other, a_cols)
    pieces = pieces_along(update, "depth")
    inverse, below = factor(where, block, block_other)
    return solve(where, pieces, inverse, below)


def solution(mesh):
    split_mesh = Mesh(
        mesh.devices.reshape(mesh.shape["row"], 8, 2, mesh.shape["depth"]),
        ("row", "col_0", "col_1", "depth"),
    )

    placed = (P(ROW_COL, None), P(ROW_COL, "depth"))
    return jax.shard_map(
        body, mesh=split_mesh, in_specs=placed, out_specs=P(ROW_COL, None), check_vma=False
    )
```

```python
import jax, jax.numpy as jnp
from jax import lax
from jax.experimental import pallas as pl
from jax.experimental.pallas import tpu as pltpu
NB=512
H=256
CENTRE, RADIUS = 7.0, 5.0
GRANT = 24 * 2**20
CHEB = 6
NEWTON = 2


def dims(ta, tb):
    return (((0 if ta else 1,), (1 if tb else 0,)), ((), ()))


def dot1(a, b, ta=False, tb=False):
    return lax.dot_general(a, b, dims(ta, tb), preferred_element_type=jnp.float32)


def split(a):
    hi = a.astype(jnp.bfloat16)
    return hi, (a - hi.astype(jnp.float32)).astype(jnp.bfloat16)


def dot3(a, b, ta=False, tb=False):
    (ah, al), (bh, bl) = a, b
    return dot1(ah, bh, ta, tb) + (dot1(ah, bl, ta, tb) + dot1(al, bh, ta, tb))


def tri(n, strict=False):
    r = lax.broadcasted_iota(jnp.int32, (n, n), 0)
    c = lax.broadcasted_iota(jnp.int32, (n, n), 1)
    return (r > c) if strict else (r >= c)


def eye(n):
    r = lax.broadcasted_iota(jnp.int32, (n, n), 0)
    c = lax.broadcasted_iota(jnp.int32, (n, n), 1)
    return (r == c)


def inverse_factor(a00, a10, a11):
    b = jnp.bfloat16
    low, ident = tri(H), eye(H).astype(jnp.float32)
    h00, h10, h11 = split(a00), split(a10), split(a11)
    b00, b10, b11 = h00[0], h10[0], h11[0]
    sigma = CENTRE / RADIUS
    rho = 1.0 / sigma
    d00 = ident * (1.0 / CENTRE); d11 = d00; d10 = jnp.zeros((H, H), jnp.float32)
    y00, y10, y11 = d00, d10, d11
    zero = jnp.zeros((H, H), jnp.float32)
    r00 = ident - jnp.where(low, a00, 0.0) * (1.0 / CENTRE)
    r10 = -a10 * (1.0 / CENTRE)
    r11 = ident - jnp.where(low, a11, 0.0) * (1.0 / CENTRE)
    for k in range(CHEB):
        nxt = 1.0 / (2.0 * sigma - rho)
        p, q = nxt * rho, 2.0 * nxt / RADIUS
        rho = nxt
        d00, d10, d11 = p * d00 + q * r00, p * d10 + q * r10, p * d11 + q * r11
        y00, y10, y11 = y00 + d00, y10 + d10, y11 + d11
        if k < CHEB - 1:
            v00, v10, v11 = y00.astype(b), y10.astype(b), y11.astype(b)
            r00 = ident - jnp.where(low, dot1(v00, b00), 0.0)
            r10 = -(dot1(v10, b00) + dot1(v11, b10))
            r11 = ident - jnp.where(low, dot1(v10, b10, False, True) + dot1(v11, b11), 0.0)
    s0 = lax.rsqrt(jnp.sum(y00 * ident, axis=1, keepdims=True))
    s1 = lax.rsqrt(jnp.sum(y11 * ident, axis=1, keepdims=True))
    x00, x10, x11 = y00 * s0, y10 * s1, y11 * s1
    half = jnp.where(tri(H, True), 1.0, 0.5 * ident)
    for _ in range(NEWTON):
        t00, t10, t11 = split(x00), split(x10), split(x11)
        w00 = split(dot3(t00, h00))
        w10 = split(dot3(t10, h00) + dot3(t11, h10))
        w11 = split(dot3(t10, h10, False, True) + dot3(t11, h11))
        e00 = ((dot3(w00, t00, False, True) - ident) * half).astype(b)
        e10 = dot3(w10, t00, False, True).astype(b)
        e11 = ((dot3(w10, t10, False, True) + dot3(w11, t11, False, True) - ident) * half).astype(b)
        x10 = x10 - (dot1(e10, t00[0]) + dot1(e11, t10[0]))
        x00 = x00 - dot1(e00, t00[0])
        x11 = x11 - dot1(e11, t11[0])
    return x00, x10, x11


VMEM = pl.BlockSpec(memory_space=pltpu.VMEM)
SMEM = pl.BlockSpec(memory_space=pltpu.SMEM)
F32 = jnp.float32


CHUNK = 160
PIECE = CHUNK // 4


def block_kernel(where_ref, own, other, a_ref, *refs):
    outs, part = refs[:4], refs[4]
    first, y = where_ref[0] == 0, where_ref[1]
    n = H // 4
    t0, t1 = split(own[:H, :]), split(own[H:, :])
    part[:, :H] = -dot3(t0, t0, False, True)
    part[:, H : 2 * H] = -dot3(t1, t0, False, True)
    part[:, 2 * H : 3 * H] = -dot3(t1, t1, False, True)

    def rows_of(start, size):
        return pl.ds(pl.multiple_of(start + y * n, size), size)

    above, below = rows_of(0, n), rows_of(H, n)
    out = outs[0]

    @pl.when(first)
    def _():
        q = split(other[:H, :])
        part[:, 3 * H : 4 * H] = -dot3(t0, q, False, True)
        part[:, 4 * H :] = -dot3(t1, q, False, True)
        out[:n, :H] = a_ref[above, :H]
        out[:n, H:] = a_ref[below, :H]
        out[n : 2 * n, :H] = a_ref[below, H:NB]
        out[n : 2 * n, H:] = a_ref[above, NB : NB + H]
        out[2 * n :, :H] = a_ref[rows_of(H, n // 2), NB : NB + H]
        out[2 * n :, H:] = a_ref[rows_of(H + n // 2, n // 2), NB : NB + H]

    @pl.when(jnp.logical_not(first))
    def _():
        part[:, 3 * H : 4 * H] = -dot3(t1, split(other[:H, :]), False, True)
        part[:, 4 * H :] = -dot3(t1, split(other[H:, :]), False, True)
        out[:n, :H] = a_ref[above, NB : NB + H]
        out[:n, H:] = a_ref[below, NB : NB + H]
        out[n : 2 * n, :H] = a_ref[below, NB + H :]
        out[n : 2 * n, H:] = a_ref[below, :H]
        out[2 * n :, :H] = a_ref[rows_of(H, n // 2), H:NB]
        out[2 * n :, H:] = a_ref[rows_of(H + n // 2, n // 2), H:NB]

    for s in range(4):
        q = y ^ s
        rows = pl.ds(pl.multiple_of(q * n, n), n)
        top = pl.ds(pl.multiple_of(q * n, n // 2), n // 2)
        bottom = pl.ds(pl.multiple_of(q * n + n // 2, n // 2), n // 2)
        new = part[rows, :NB], part[rows, NB : 2 * NB], part[top, 4 * H :], part[bottom, 4 * H :]
        to = (
            (slice(0, n), slice(0, NB)),
            (slice(n, 2 * n), slice(0, NB)),
            (slice(2 * n, CHUNK), slice(0, H)),
            (slice(2 * n, CHUNK), slice(H, NB)),
        )
        for place, value in zip(to, new):
            outs[s][place] = value + out[place] if s == 0 else value


def lay_out(m, got):
    n = H // 4
    for y in range(4):
        for x in range(4):
            for i in range(x * PIECE, (x + 1) * PIECE, 8):
                v = got[x, y, i - x * PIECE : i - x * PIECE + 8, :]
                if i < 2 * n:
                    part, row = i // n, i % n
                    m[y * n + row : y * n + row + 8, part * NB : (part + 1) * NB] = v
                else:
                    row = y * n + i - 2 * n
                    m[row : row + 8, 4 * H :] = v[:, :H]
                    m[row + n // 2 : row + n // 2 + 8, 4 * H :] = v[:, H:]


def block_parts(where, own, other, a_cols):
    return pl.pallas_call(
        block_kernel,
        out_shape=(jax.ShapeDtypeStruct((CHUNK, NB), F32),) * 4,
        in_specs=[SMEM, VMEM, VMEM, VMEM],
        out_specs=(VMEM,) * 4,
        scratch_shapes=[pltpu.VMEM((H, 5 * H), F32)],
        compiler_params=pltpu.CompilerParams(vmem_limit_bytes=GRANT),
        cost_estimate=pl.CostEstimate(flops=10**9, bytes_accessed=2**22, transcendentals=0),
        name="block_parts",
    )(where, own, other, a_cols)


def factor_kernel(where_ref, own, other, x_ref, l_ref, m0, m1):
    @pl.when(where_ref[0] == 0)
    def _():
        lay_out(m0, own)
        lay_out(m1, other)

    @pl.when(where_ref[0] != 0)
    def _():
        lay_out(m0, other)
        lay_out(m1, own)

    def tile(m, i):
        return m[:, i * H : (i + 1) * H]

    def put(i, x00, x10, x11):
        x_ref[i, :H, :H] = x00
        x_ref[i, :H, H:] = jnp.zeros((H, H), F32)
        x_ref[i, H:, :H] = x10
        x_ref[i, H:, H:] = x11

    x00, x10, x11 = inverse_factor(tile(m0, 0), tile(m0, 1), tile(m0, 2))
    put(0, x00, x10, x11)
    t00, t10, t11 = split(x00), split(x10), split(x11)
    for j, m in enumerate((m0, m1)):
        top, bot = split(tile(m, 3)), split(tile(m, 4))
        l_ref[:H, j * H : (j + 1) * H] = dot3(t00, top, False, j == 1)
        l_ref[H:, j * H : (j + 1) * H] = dot3(t10, top, False, j == 1) + dot3(t11, bot, False, j == 1)
    p0, p1 = split(l_ref[:, :H]), split(l_ref[:, H:])
    c00 = tile(m1, 0) - dot3(p0, p0, True, False)
    c10 = tile(m1, 1) - dot3(p1, p0, True, False)
    c11 = tile(m1, 2) - dot3(p1, p1, True, False)
    put(1, *inverse_factor(c00, c10, c11))


def factor(where, own, other):
    return pl.pallas_call(
        factor_kernel,
        out_shape=(jax.ShapeDtypeStruct((2, NB, NB), F32), jax.ShapeDtypeStruct((NB, NB), F32)),
        in_specs=[SMEM] + [VMEM] * 2,
        out_specs=(VMEM,) * 2,
        scratch_shapes=[pltpu.VMEM((H, 5 * H), F32)] * 2,
        compiler_params=pltpu.CompilerParams(vmem_limit_bytes=GRANT),
        cost_estimate=pl.CostEstimate(flops=5 * 10**9, bytes_accessed=2**23, transcendentals=0),
        name="factor",
    )(where, own, other)


def put_split(hi, lo, row, column, src, low=0):
    step = 32
    for r in range(0, src.shape[0], step):
        v = src[r : r + step, :]
        columns = slice(column, column + src.shape[1])
        hi[row + r : row + r + step, columns], lo[low + row + r : low + row + r + step, columns] = split(v)


def rows_kernel(p0, p1a, p1b, p2a, p2b, p3a, p3b, hi, lo):
    put_split(hi, lo, 0, 0, p0)
    for t, (above, below) in enumerate(((p1b, p1a), (p2a, p2b), (p3a, p3b))):
        put_split(hi, lo, 0, (t + 1) * NB, above)
        put_split(hi, lo, H, (t + 1) * NB, below)


def split_rows(*past):
    return pl.pallas_call(
        rows_kernel,
        out_shape=(jax.ShapeDtypeStruct((NB, 4 * NB), jnp.bfloat16),) * 2,
        in_specs=[VMEM] * 7,
        out_specs=(VMEM,) * 2,
        compiler_params=pltpu.CompilerParams(vmem_limit_bytes=GRANT),
        cost_estimate=pl.CostEstimate(flops=10**8, bytes_accessed=2**23, transcendentals=0),
        name="split_rows",
    )(*past)


def update_kernel(where_ref, ph, pl_, own, other, a_ref, out, th):
    core, y = where_ref[0], where_ref[1]
    n = 128
    for t in range(4):
        put_split(th, th, 0, t * NB, own.at[t * n : (t + 1) * n, :], H)
        put_split(th, th, n, t * NB, other.at[t * n : (t + 1) * n, :], H)
    both = dot1(ph[...], th[...], False, True)
    total = both[:, :H] + (both[:, H:] + dot1(pl_[...], th[:H, :], False, True))
    for i, half in enumerate((core, 1 - core)):
        columns = pl.ds(pl.multiple_of(half * NB + y * n, n), n)
        out[:, pl.ds(pl.multiple_of(half * n, n), n)] = a_ref[:, columns] - total[:, i * n : (i + 1) * n]


def update_part(where, rows, own, other, a_cols):
    return pl.pallas_call(
        update_kernel,
        out_shape=jax.ShapeDtypeStruct((NB, 256), F32),
        in_specs=[SMEM] + [VMEM] * 5,
        out_specs=VMEM,
        scratch_shapes=[pltpu.VMEM((NB, 4 * NB), jnp.bfloat16)],
        compiler_params=pltpu.CompilerParams(vmem_limit_bytes=GRANT),
        cost_estimate=pl.CostEstimate(flops=10**9, bytes_accessed=2**22, transcendentals=0),
        name="update_part",
    )(where, *rows, own, other, a_cols)


def solve_kernel(where_ref, u0, u1, u2, u3, x_ref, l_ref, out, s1, s2, h, lo, w, v):
    y, position = where_ref[1], where_ref[2]
    n = 128
    for u, piece in enumerate((u0, u1, u2, u3)):
        columns = pl.ds(pl.multiple_of((y ^ u) * n, n), n)
        s1[:, columns] = piece[:, :n]
        s2[:, columns] = piece[:, n:]

    def product(left, right, transposed):
        put_split(h, lo, 0, 0, left)
        put_split(w, v, 0, 0, right)
        return dot3((h[...], lo[...]), (w[...], v[...]), False, transposed)

    def keep(start):
        rows = position * NB + lax.broadcasted_iota(jnp.int32, (NB, NB), 0)
        columns = slice(start, start + NB)
        kept = rows >= start + lax.broadcasted_iota(jnp.int32, (NB, NB), 1)
        out[:, columns] = jnp.where(kept, out[:, columns], 0.0)

    out[:, :NB] = product(s1, x_ref.at[0], True)
    s2[...] = s2[...] - product(out.at[:, :NB], l_ref, False)
    out[:, NB:] = product(s2, x_ref.at[1], True)

    @pl.when(position < 2)
    def _():
        keep(0)
        keep(NB)


def solve(where, pieces, inverse, below):
    return pl.pallas_call(
        solve_kernel,
        out_shape=jax.ShapeDtypeStruct((NB, 2 * NB), F32),
        in_specs=[SMEM] + [VMEM] * 6,
        out_specs=VMEM,
        scratch_shapes=[pltpu.VMEM((NB, NB), F32)] * 2 + [pltpu.VMEM((NB, NB), jnp.bfloat16)] * 4,
        compiler_params=pltpu.CompilerParams(vmem_limit_bytes=GRANT),
        cost_estimate=pl.CostEstimate(flops=10**9, bytes_accessed=2**22, transcendentals=0),
        name="solve",
    )(where, *pieces, inverse, below)


from jax.sharding import Mesh
from jax.sharding import PartitionSpec as P

ROW_COL = ("row", "col_0", "col_1")
PLANE = ("row", "col_0")
BOX = ("row", "col_0", "depth")
TRADE = False


def send(v, axis, pairs, one_way=False):
    if one_way and TRADE:
        pairs = pairs + [(b, a) for a, b in pairs]
    return lax.ppermute(v, axis, pairs)


def swap_core(v):
    return send(v, "col_1", [(0, 1), (1, 0)])


def exchange(v, axis, bits):
    return send(v, axis, [(i, i ^ bits) for i in range(4)])


def in_order(pieces, me):
    low, high = (me & 1) == 1, (me >> 1) == 1
    p0, p1, p2, p3 = pieces
    p0, p1 = jnp.where(low, p1, p0), jnp.where(low, p0, p1)
    p2, p3 = jnp.where(low, p3, p2), jnp.where(low, p2, p3)
    p0, p2 = jnp.where(high, p2, p0), jnp.where(high, p0, p2)
    p1, p3 = jnp.where(high, p3, p1), jnp.where(high, p1, p3)
    return jnp.concatenate([p0, p1, p2, p3])


def pieces_along(v, axis):
    return [v] + [exchange(v, axis, s) for s in (1, 2, 3)]


def chunk_of(v, j):
    n = v.shape[0] // 4
    return lax.dynamic_slice_in_dim(v, j * n, n)


def spread_z(v, z):
    a = send(v, "col_0", [(0, 3)], True) + send(v, "col_0", [(0, 5)], True)
    v = jnp.where(z == 0, v, a)
    b = send(v, "col_0", [(0, 1), (3, 4), (5, 6)], True) + send(v, "col_0", [(0, 7), (3, 2)], True)
    return jnp.where((z == 0) | (z == 3) | (z == 5), v, b)


def body(a_cols, past):
    x, z = lax.axis_index("row"), lax.axis_index("col_0")
    core, y = lax.axis_index("col_1"), lax.axis_index("depth")
    root = (x == 0) & (z == 0)
    where = jnp.stack([core, y, lax.axis_index(ROW_COL)]).astype(jnp.int32)

    other = swap_core(past)
    got = 0.0
    for s in (1, 2, 3):
        pairs = [(d, 32 * s + (d ^ s)) for d in range(4)]
        got = got + send(chunk_of(past, y ^ s), BOX, pairs, True)
    top = jnp.where(root, chunk_of(past, y), got)

    parts = block_parts(where, past, other, a_cols)
    block = parts[0]
    for s in (1, 2, 3):
        block = block + send(parts[s], BOX, [(d, d ^ s) for d in range(4)])

    near1, near3 = exchange(past[H:], "depth", 1), exchange(past[:H], "depth", 3)
    far1, far3 = exchange(near3, "depth", 1), exchange(near1, "depth", 3)
    rest1, rest3 = exchange(past[:H], "depth", 1), exchange(past[H:], "depth", 3)
    rows = split_rows(past, near1, rest1, far1, far3, near3, rest3)

    got = 0.0
    for p in (1, 2, 3):
        got = got + send(block[p * PIECE : (p + 1) * PIECE], PLANE, [(0, 8 * p)], True)
    both = spread_z(jnp.concatenate([top, jnp.where(root, block[:PIECE], got)]), z)

    top = in_order(pieces_along(both[:128], "row"), x)
    top_other = swap_core(top)

    block = in_order(pieces_along(both[128:][None], "depth"), y)
    block = in_order(pieces_along(block[None], "row"), x)
    block_other = swap_core(block)

    update = update_part(where, rows, top, top_other, a_cols)
    pieces = pieces_along(update, "depth")
    inverse, below = factor(where, block, block_other)
    return solve(where, pieces, inverse, below)


def solution(mesh):
    split_mesh = Mesh(
        mesh.devices.reshape(mesh.shape["row"], 8, 2, mesh.shape["depth"]),
        ("row", "col_0", "col_1", "depth"),
    )

    placed = (P(ROW_COL, None), P(ROW_COL, "depth"))
    return jax.shard_map(body, mesh=split_mesh, in_specs=placed, out_specs=P(ROW_COL, None), check_vma=False)
```

```python
import jax, jax.numpy as jnp
from jax import lax
from jax.experimental import pallas as pl
from jax.experimental.pallas import tpu as pltpu
NB=512
H=256
CENTRE, RADIUS = 7.0, 5.0
GRANT = 24 * 2**20
CHEB = 6
NEWTON = 2


def dims(ta, tb):
    return (((0 if ta else 1,), (1 if tb else 0,)), ((), ()))


def dot1(a, b, ta=False, tb=False):
    return lax.dot_general(a, b, dims(ta, tb), preferred_element_type=jnp.float32)


def split(a):
    hi = a.astype(jnp.bfloat16)
    return hi, (a - hi.astype(jnp.float32)).astype(jnp.bfloat16)


def dot3(a, b, ta=False, tb=False):
    (ah, al), (bh, bl) = a, b
    return dot1(ah, bh, ta, tb) + (dot1(ah, bl, ta, tb) + dot1(al, bh, ta, tb))


def tri(n, strict=False):
    r = lax.broadcasted_iota(jnp.int32, (n, n), 0)
    c = lax.broadcasted_iota(jnp.int32, (n, n), 1)
    return (r > c) if strict else (r >= c)


def eye(n):
    r = lax.broadcasted_iota(jnp.int32, (n, n), 0)
    c = lax.broadcasted_iota(jnp.int32, (n, n), 1)
    return (r == c)


def inverse_factor(a00, a10, a11):
    b = jnp.bfloat16
    low, ident = tri(H), eye(H).astype(jnp.float32)
    h00, h10, h11 = split(a00), split(a10), split(a11)
    b00, b10, b11 = h00[0], h10[0], h11[0]
    sigma = CENTRE / RADIUS
    rho = 1.0 / sigma
    d00 = ident * (1.0 / CENTRE); d11 = d00; d10 = jnp.zeros((H, H), jnp.float32)
    y00, y10, y11 = d00, d10, d11
    zero = jnp.zeros((H, H), jnp.float32)
    r00 = ident - jnp.where(low, a00, 0.0) * (1.0 / CENTRE)
    r10 = -a10 * (1.0 / CENTRE)
    r11 = ident - jnp.where(low, a11, 0.0) * (1.0 / CENTRE)
    for k in range(CHEB):
        nxt = 1.0 / (2.0 * sigma - rho)
        p, q = nxt * rho, 2.0 * nxt / RADIUS
        rho = nxt
        d00, d10, d11 = p * d00 + q * r00, p * d10 + q * r10, p * d11 + q * r11
        y00, y10, y11 = y00 + d00, y10 + d10, y11 + d11
        if k < CHEB - 1:
            v00, v10, v11 = y00.astype(b), y10.astype(b), y11.astype(b)
            r00 = ident - jnp.where(low, dot1(v00, b00), 0.0)
            r10 = -(dot1(v10, b00) + dot1(v11, b10))
            r11 = ident - jnp.where(low, dot1(v10, b10, False, True) + dot1(v11, b11), 0.0)
    s0 = lax.rsqrt(jnp.sum(y00 * ident, axis=1, keepdims=True))
    s1 = lax.rsqrt(jnp.sum(y11 * ident, axis=1, keepdims=True))
    x00, x10, x11 = y00 * s0, y10 * s1, y11 * s1
    half = jnp.where(tri(H, True), 1.0, 0.5 * ident)
    for _ in range(NEWTON):
        t00, t10, t11 = split(x00), split(x10), split(x11)
        w00 = split(dot3(t00, h00))
        w10 = split(dot3(t10, h00) + dot3(t11, h10))
        w11 = split(dot3(t10, h10, False, True) + dot3(t11, h11))
        e00 = ((dot3(w00, t00, False, True) - ident) * half).astype(b)
        e10 = dot3(w10, t00, False, True).astype(b)
        e11 = ((dot3(w10, t10, False, True) + dot3(w11, t11, False, True) - ident) * half).astype(b)
        x10 = x10 - (dot1(e10, t00[0]) + dot1(e11, t10[0]))
        x00 = x00 - dot1(e00, t00[0])
        x11 = x11 - dot1(e11, t11[0])
    return x00, x10, x11


VMEM = pl.BlockSpec(memory_space=pltpu.VMEM)
SMEM = pl.BlockSpec(memory_space=pltpu.SMEM)
HBM = pl.BlockSpec(memory_space=pltpu.HBM)
F32 = jnp.float32


CHUNK = 160
PIECE = CHUNK // 4


def block_kernel(where_ref, own, other, a_ref, *refs):
    outs, part, a_rows, sems = refs[:4], refs[4], refs[5], refs[6]
    first, y = where_ref[0] == 0, where_ref[1]
    n = H // 4

    def rows_of(start, size):
        return pl.ds(pl.multiple_of(start + y * n, size), size)

    def copies(places):
        to = ((0, n, 0), (0, n, H), (n, n, 0), (n, n, H), (2 * n, n // 2, 0), (2 * n, n // 2, H))
        return [
            pltpu.make_async_copy(
                a_ref.at[rows_of(start, size), column : column + H],
                a_rows.at[row : row + size, side : side + H],
                sems.at[i],
            )
            for i, ((row, size, side), (start, column)) in enumerate(zip(to, places))
        ]

    places = (
        ((0, 0), (H, 0), (H, H), (0, NB), (H, NB), (H + n // 2, NB)),
        ((0, NB), (H, NB), (H, NB + H), (H, 0), (H, H), (H + n // 2, H)),
    )

    @pl.when(first)
    def _():
        for copy in copies(places[0]):
            copy.start()

    @pl.when(jnp.logical_not(first))
    def _():
        for copy in copies(places[1]):
            copy.start()

    t0, t1 = split(own[:H, :]), split(own[H:, :])
    part[:, :H] = -dot3(t0, t0, False, True)
    part[:, H : 2 * H] = -dot3(t1, t0, False, True)
    part[:, 2 * H : 3 * H] = -dot3(t1, t1, False, True)

    @pl.when(first)
    def _():
        q = split(other[:H, :])
        part[:, 3 * H : 4 * H] = -dot3(t0, q, False, True)
        part[:, 4 * H :] = -dot3(t1, q, False, True)
        for copy in copies(places[0]):
            copy.wait()

    @pl.when(jnp.logical_not(first))
    def _():
        part[:, 3 * H : 4 * H] = -dot3(t1, split(other[:H, :]), False, True)
        part[:, 4 * H :] = -dot3(t1, split(other[H:, :]), False, True)
        for copy in copies(places[1]):
            copy.wait()

    for s in range(4):
        q = y ^ s
        rows = pl.ds(pl.multiple_of(q * n, n), n)
        top = pl.ds(pl.multiple_of(q * n, n // 2), n // 2)
        bottom = pl.ds(pl.multiple_of(q * n + n // 2, n // 2), n // 2)
        new = part[rows, :NB], part[rows, NB : 2 * NB], part[top, 4 * H :], part[bottom, 4 * H :]
        to = (
            (slice(0, n), slice(0, NB)),
            (slice(n, 2 * n), slice(0, NB)),
            (slice(2 * n, CHUNK), slice(0, H)),
            (slice(2 * n, CHUNK), slice(H, NB)),
        )
        for place, value in zip(to, new):
            outs[s][place] = value + a_rows[place] if s == 0 else value


def lay_out(m, got):
    n = H // 4
    for y in range(4):
        for x in range(4):
            for i in range(x * PIECE, (x + 1) * PIECE, 8):
                v = got[x, y, i - x * PIECE : i - x * PIECE + 8, :]
                if i < 2 * n:
                    part, row = i // n, i % n
                    m[y * n + row : y * n + row + 8, part * NB : (part + 1) * NB] = v
                else:
                    row = y * n + i - 2 * n
                    m[row : row + 8, 4 * H :] = v[:, :H]
                    m[row + n // 2 : row + n // 2 + 8, 4 * H :] = v[:, H:]


def block_parts(where, own, other, a_cols):
    return pl.pallas_call(
        block_kernel,
        out_shape=(jax.ShapeDtypeStruct((CHUNK, NB), F32),) * 4,
        in_specs=[SMEM, VMEM, VMEM, HBM],
        out_specs=(VMEM,) * 4,
        scratch_shapes=[
            pltpu.VMEM((H, 5 * H), F32),
            pltpu.VMEM((CHUNK, NB), F32),
            pltpu.SemaphoreType.DMA((6,)),
        ],
        compiler_params=pltpu.CompilerParams(vmem_limit_bytes=GRANT),
        cost_estimate=pl.CostEstimate(flops=10**9, bytes_accessed=2**22, transcendentals=0),
        name="block_parts",
    )(where, own, other, a_cols)


def factor_kernel(where_ref, own, other, x_ref, l_ref, m0, m1):
    @pl.when(where_ref[0] == 0)
    def _():
        lay_out(m0, own)
        lay_out(m1, other)

    @pl.when(where_ref[0] != 0)
    def _():
        lay_out(m0, other)
        lay_out(m1, own)

    def tile(m, i):
        return m[:, i * H : (i + 1) * H]

    def put(i, x00, x10, x11):
        x_ref[i, :H, :H] = x00
        x_ref[i, :H, H:] = jnp.zeros((H, H), F32)
        x_ref[i, H:, :H] = x10
        x_ref[i, H:, H:] = x11

    x00, x10, x11 = inverse_factor(tile(m0, 0), tile(m0, 1), tile(m0, 2))
    put(0, x00, x10, x11)
    t00, t10, t11 = split(x00), split(x10), split(x11)
    for j, m in enumerate((m0, m1)):
        top, bot = split(tile(m, 3)), split(tile(m, 4))
        l_ref[:H, j * H : (j + 1) * H] = dot3(t00, top, False, j == 1)
        l_ref[H:, j * H : (j + 1) * H] = dot3(t10, top, False, j == 1) + dot3(t11, bot, False, j == 1)
    p0, p1 = split(l_ref[:, :H]), split(l_ref[:, H:])
    c00 = tile(m1, 0) - dot3(p0, p0, True, False)
    c10 = tile(m1, 1) - dot3(p1, p0, True, False)
    c11 = tile(m1, 2) - dot3(p1, p1, True, False)
    put(1, *inverse_factor(c00, c10, c11))


def factor(where, own, other):
    return pl.pallas_call(
        factor_kernel,
        out_shape=(jax.ShapeDtypeStruct((2, NB, NB), F32), jax.ShapeDtypeStruct((NB, NB), F32)),
        in_specs=[SMEM] + [VMEM] * 2,
        out_specs=(VMEM,) * 2,
        scratch_shapes=[pltpu.VMEM((H, 5 * H), F32)] * 2,
        compiler_params=pltpu.CompilerParams(vmem_limit_bytes=GRANT),
        cost_estimate=pl.CostEstimate(flops=5 * 10**9, bytes_accessed=2**23, transcendentals=0),
        name="factor",
    )(where, own, other)


def put_split(hi, lo, row, column, src, low=0):
    step = 32
    for r in range(0, src.shape[0], step):
        v = src[r : r + step, :]
        columns = slice(column, column + src.shape[1])
        hi[row + r : row + r + step, columns], lo[low + row + r : low + row + r + step, columns] = split(v)


def rows_kernel(p0, p1a, p1b, p3a, p3b, hi, lo):
    put_split(hi, lo, 0, 0, p0)
    for t, (above, below) in enumerate(((p1b, p1a), (p3a, p3b))):
        put_split(hi, lo, 0, (t + 1) * NB, above)
        put_split(hi, lo, H, (t + 1) * NB, below)


def split_rows(*past):
    return pl.pallas_call(
        rows_kernel,
        out_shape=(jax.ShapeDtypeStruct((NB, 3 * NB), jnp.bfloat16),) * 2,
        in_specs=[VMEM] * 5,
        out_specs=(VMEM,) * 2,
        compiler_params=pltpu.CompilerParams(vmem_limit_bytes=GRANT),
        cost_estimate=pl.CostEstimate(flops=10**8, bytes_accessed=2**23, transcendentals=0),
        name="split_rows",
    )(*past)


def update_kernel(where_ref, ph, pl_, far1, far3, own, other, a_ref, out, th, fh, fl):
    core, y = where_ref[0], where_ref[1]
    n = 128
    for place, t in enumerate((0, 1, 3, 2)):
        put_split(th, th, 0, place * NB, own.at[t * n : (t + 1) * n, :], H)
        put_split(th, th, n, place * NB, other.at[t * n : (t + 1) * n, :], H)
    put_split(fh, fl, 0, 0, far1)
    put_split(fh, fl, H, 0, far3)

    def product(hi, lo, columns):
        both = dot1(hi[...], th[:, columns], False, True)
        return both[:, :H] + (both[:, H:] + dot1(lo[...], th[:H, columns], False, True))

    total = product(ph, pl_, slice(0, 3 * NB)) + product(fh, fl, slice(3 * NB, 4 * NB))
    for i, half in enumerate((core, 1 - core)):
        columns = pl.ds(pl.multiple_of(half * NB + y * n, n), n)
        out[:, pl.ds(pl.multiple_of(half * n, n), n)] = a_ref[:, columns] - total[:, i * n : (i + 1) * n]


def update_part(where, rows, far, own, other, a_cols):
    return pl.pallas_call(
        update_kernel,
        out_shape=jax.ShapeDtypeStruct((NB, 256), F32),
        in_specs=[SMEM] + [VMEM] * 7,
        out_specs=VMEM,
        scratch_shapes=[pltpu.VMEM((NB, c * NB), jnp.bfloat16) for c in (4, 1, 1)],
        compiler_params=pltpu.CompilerParams(vmem_limit_bytes=GRANT),
        cost_estimate=pl.CostEstimate(flops=10**9, bytes_accessed=2**22, transcendentals=0),
        name="update_part",
    )(where, *rows, *far, own, other, a_cols)


def solve_kernel(where_ref, u0, u1, u2, u3, x_ref, l_ref, out, s1, s2, h, lo, w, v):
    y, position = where_ref[1], where_ref[2]
    n = 128
    for u, piece in enumerate((u0, u1, u2, u3)):
        columns = pl.ds(pl.multiple_of((y ^ u) * n, n), n)
        s1[:, columns] = piece[:, :n]
        s2[:, columns] = piece[:, n:]

    def product(left, right, transposed):
        put_split(h, lo, 0, 0, left)
        put_split(w, v, 0, 0, right)
        return dot3((h[...], lo[...]), (w[...], v[...]), False, transposed)

    def keep(start):
        rows = position * NB + lax.broadcasted_iota(jnp.int32, (NB, NB), 0)
        columns = slice(start, start + NB)
        kept = rows >= start + lax.broadcasted_iota(jnp.int32, (NB, NB), 1)
        out[:, columns] = jnp.where(kept, out[:, columns], 0.0)

    out[:, :NB] = product(s1, x_ref.at[0], True)
    s2[...] = s2[...] - product(out.at[:, :NB], l_ref, False)
    out[:, NB:] = product(s2, x_ref.at[1], True)

    @pl.when(position < 2)
    def _():
        keep(0)
        keep(NB)


def solve(where, pieces, inverse, below):
    return pl.pallas_call(
        solve_kernel,
        out_shape=jax.ShapeDtypeStruct((NB, 2 * NB), F32),
        in_specs=[SMEM] + [VMEM] * 6,
        out_specs=VMEM,
        scratch_shapes=[pltpu.VMEM((NB, NB), F32)] * 2 + [pltpu.VMEM((NB, NB), jnp.bfloat16)] * 4,
        compiler_params=pltpu.CompilerParams(vmem_limit_bytes=GRANT),
        cost_estimate=pl.CostEstimate(flops=10**9, bytes_accessed=2**22, transcendentals=0),
        name="solve",
    )(where, *pieces, inverse, below)


from jax.sharding import Mesh
from jax.sharding import PartitionSpec as P

ROW_COL = ("row", "col_0", "col_1")
PLANE = ("row", "col_0")
BOX = ("row", "col_0", "depth")
TRADE = False


def send(v, axis, pairs, one_way=False):
    if one_way and TRADE:
        pairs = pairs + [(b, a) for a, b in pairs]
    return lax.ppermute(v, axis, pairs)


def swap_core(v):
    return send(v, "col_1", [(0, 1), (1, 0)])


def exchange(v, axis, bits):
    return send(v, axis, [(i, i ^ bits) for i in range(4)])


def in_order(pieces, me):
    low, high = (me & 1) == 1, (me >> 1) == 1
    p0, p1, p2, p3 = pieces
    p0, p1 = jnp.where(low, p1, p0), jnp.where(low, p0, p1)
    p2, p3 = jnp.where(low, p3, p2), jnp.where(low, p2, p3)
    p0, p2 = jnp.where(high, p2, p0), jnp.where(high, p0, p2)
    p1, p3 = jnp.where(high, p3, p1), jnp.where(high, p1, p3)
    return jnp.concatenate([p0, p1, p2, p3])


def pieces_along(v, axis):
    return [v] + [exchange(v, axis, s) for s in (1, 2, 3)]


def chunk_of(v, j):
    n = v.shape[0] // 4
    return lax.dynamic_slice_in_dim(v, j * n, n)


def spread_z(v, z):
    a = send(v, "col_0", [(0, 3)], True) + send(v, "col_0", [(0, 5)], True)
    v = jnp.where(z == 0, v, a)
    b = send(v, "col_0", [(0, 1), (3, 4), (5, 6)], True) + send(v, "col_0", [(0, 7), (3, 2)], True)
    return jnp.where((z == 0) | (z == 3) | (z == 5), v, b)


def body(a_cols, past):
    x, z = lax.axis_index("row"), lax.axis_index("col_0")
    core, y = lax.axis_index("col_1"), lax.axis_index("depth")
    root = (x == 0) & (z == 0)
    where = jnp.stack([core, y, lax.axis_index(ROW_COL)]).astype(jnp.int32)

    other = swap_core(past)
    got = 0.0
    for s in (1, 2, 3):
        pairs = [(d, 32 * s + (d ^ s)) for d in range(4)]
        got = got + send(chunk_of(past, y ^ s), BOX, pairs, True)
    top = jnp.where(root, chunk_of(past, y), got)

    parts = block_parts(where, past, other, a_cols)
    block = parts[0]
    for s in (1, 2, 3):
        block = block + send(parts[s], BOX, [(d, d ^ s) for d in range(4)])

    near1, near3 = exchange(past[H:], "depth", 1), exchange(past[:H], "depth", 3)
    far1, far3 = exchange(near3, "depth", 1), exchange(near1, "depth", 3)
    rest1, rest3 = exchange(past[:H], "depth", 1), exchange(past[H:], "depth", 3)
    rows = split_rows(past, near1, rest1, near3, rest3)

    got = 0.0
    for p in (1, 2, 3):
        got = got + send(block[p * PIECE : (p + 1) * PIECE], PLANE, [(0, 8 * p)], True)
    both = spread_z(jnp.concatenate([top, jnp.where(root, block[:PIECE], got)]), z)

    top = in_order(pieces_along(both[:128], "row"), x)
    top_other = swap_core(top)

    block = in_order(pieces_along(both[128:][None], "depth"), y)
    block = in_order(pieces_along(block[None], "row"), x)
    block_other = swap_core(block)

    update = update_part(where, rows, (far1, far3), top, top_other, a_cols)
    pieces = pieces_along(update, "depth")
    inverse, below = factor(where, block, block_other)
    return solve(where, pieces, inverse, below)


def solution(mesh):
    split_mesh = Mesh(
        mesh.devices.reshape(mesh.shape["row"], 8, 2, mesh.shape["depth"]),
        ("row", "col_0", "col_1", "depth"),
    )

    placed = (P(ROW_COL, None), P(ROW_COL, "depth"))
    return jax.shard_map(body, mesh=split_mesh, in_specs=placed, out_specs=P(ROW_COL, None), check_vma=False)
```
